256 devices in a mesh: seg: 32 (over y, x, core), coil: 8 (over z).
Axes of the slice: x: 4, y: 4, z: 8, core: 2. Of those that a mesh axis runs over, the one named last changes fastest.
Arguments:
- measured: float32 [64, 2, 32, 8, 512], P('seg', None, 'coil'), may hold values from -0.4 to 0.4
- forward_kernel: float32 [64, 2, 256, 128], P('seg', None, None, 'coil'), may hold values from -0.375 to 0.375
- backward_kernel: float32 [64, 2, 256, 128], P('seg', None, None, 'coil'), may hold values from -0.375 to 0.375
- line_offsets: int32 [64, 2, 4], P('seg'), may hold values from 0 to 7
Outputs:
- forward: float32 [64, 2, 32, 8, 512], P('seg', None, 'coil')
- result: float32 [64, 2, 32, 8, 512], P('seg', None, 'coil')
The draws below stay inside these ranges and needn't reach their ends.
All inputs are finite; a program needn't handle non-finite values.
Results may differ from the reference program's by a relative error of at most 0.0003.
Values sent between devices are 32-bit elements; how exact they have to be, the bound alone decides.
A program may use at most 128 MiB of HBM per device.

```python
import jax
import jax.numpy as jnp
from jax import lax

COILS = 32
X = 512
LINES = 8
J = 4
SEGS = 64
STATE = 512


def with_ends(values, key, least, high):
    longest = values.shape.index(max(values.shape))
    spots = []
    for shift in (0, 1):
        where = [jax.random.randint(jax.random.fold_in(key, axis), (), 0, length) for axis, length in enumerate(values.shape)]
        where[longest] = (where[longest] + shift) % values.shape[longest]
        spots.append(tuple(where))
    return values.at[spots[0]].set(least).at[spots[1]].set(high)


def steps_of(key, shape, pieces, low, top_value):
    level = 1.0
    for dim, blocks in pieces:
        heights = jax.random.uniform(jax.random.fold_in(jax.random.fold_in(key, 6), dim), (blocks,), jnp.float32, low / len(pieces), top_value / len(pieces))
        level = level * jnp.repeat(jnp.exp(heights), shape[dim] // blocks).reshape((-1,) + (1,) * (len(shape) - 1 - dim))
    return level


def centred(own_key, dims, scale, limit, cuts=(), held_as=jnp.bfloat16):
    level = steps_of(own_key, dims, cuts, -0.22, 0.18) if cuts else 1.0
    values = jax.random.normal(own_key, dims, jnp.float32) * scale * level
    return jnp.minimum(jnp.maximum(values, -limit), limit).astype(held_as)


def setup_inputs(seed: int = 0) -> dict:
    keys = jax.random.split(jax.random.key(seed), 5)
    measured = centred(keys[0], (SEGS, 2, COILS, LINES, X), 0.05, 0.4, ((0, 32), (2, 8)), jnp.float32)
    forward_kernel = centred(keys[1], (SEGS, 2, COILS * LINES, COILS * J), (2 * COILS * J) ** -0.5, 0.375, ((0, 32), (3, 8)), jnp.float32)
    backward_kernel = centred(keys[2], (SEGS, 2, COILS * LINES, COILS * J), (2 * COILS * J) ** -0.5, 0.375, ((0, 32), (3, 8)), jnp.float32)
    line_offsets = with_ends(jax.random.randint(keys[3], (SEGS, 2, J), 0, LINES), jax.random.fold_in(keys[3], 1), 0, LINES - 1).astype(jnp.int32)
    return {"measured": measured, "forward_kernel": forward_kernel, "backward_kernel": backward_kernel, "line_offsets": line_offsets}


PRECISE = lax.Precision.HIGHEST


def build_maps(kernel, offsets):
    blocks = kernel.shape[0]
    source_taps = offsets.shape[1]
    coil_count = kernel.shape[3] // source_taps
    line_count = kernel.shape[2] // coil_count
    line_picks = (offsets[:, :, None] == jnp.arange(line_count, dtype=jnp.int32)[None, None, :]).astype(jnp.float32)
    kernel_parts = kernel.astype(jnp.float32).reshape(blocks, 2, coil_count * line_count, coil_count, source_taps)
    spread = jnp.einsum("srocj,sjl->srocl", kernel_parts, line_picks, precision=PRECISE)
    spread = spread.reshape(blocks, 2, coil_count * line_count, coil_count * line_count)
    upper_rows = jnp.concatenate([spread[:, 0], -spread[:, 1]], axis=2)
    lower_rows = jnp.concatenate([spread[:, 1], spread[:, 0]], axis=2)
    return jnp.concatenate([upper_rows, lower_rows], axis=1)


def sweep(seg_maps, sources, backward):
    def advance(carried, inputs):
        matrix, source = inputs
        updated = jnp.dot(matrix, carried, precision=PRECISE) + source
        return updated, updated
    initial = jnp.zeros(sources.shape[1:], jnp.float32)
    _, states = lax.scan(advance, initial, (seg_maps, sources), reverse=backward)
    return states


def reference(measured, forward_kernel, backward_kernel, line_offsets):
    sources = measured.reshape(SEGS, STATE, X)
    forward = sweep(build_maps(forward_kernel, line_offsets[:, 0]), sources, False)
    result = sweep(build_maps(backward_kernel, line_offsets[:, 1]), forward, True)
    return forward.reshape(measured.shape), result.reshape(measured.shape)
```

```python
import functools

import jax
import jax.numpy as jnp
from jax import lax
from jax.experimental import pallas as pl
from jax.experimental.pallas import tpu as pltpu
from jax.sharding import Mesh
from jax.sharding import PartitionSpec as P

SEG = ("seg_0", "seg_1", "seg_2")
MESH = pl.DeviceIdType.MESH
F32 = jnp.float32
BF16 = jnp.bfloat16
LINES = 8
TAPS = 4


def split(value):
    high = value.astype(BF16)
    low = (value - high.astype(F32)).astype(BF16)
    return high, low


def product(left, right):
    lh, ll = split(left)
    rh, rl = split(right)
    dot = functools.partial(jnp.dot, preferred_element_type=F32)
    return dot(lh, rh) + (dot(lh, rl) + dot(ll, rh))


def pick(selector, value):
    high, low = split(value)
    dot = functools.partial(jnp.dot, preferred_element_type=F32)
    return dot(selector, high) + dot(selector, low)


def turned(lines):
    half = lines.shape[1] // 2
    lane = lax.broadcasted_iota(jnp.int32, lines.shape, 1)
    other = pltpu.roll(lines, half, 1)
    return jnp.where(lane < half, -other, other)


def turned_matrix(matrix):
    half = matrix.shape[1] // 2
    return jnp.concatenate([-matrix[:, half:], matrix[:, :half]], axis=1)


def apply_lines(matrix, lines):
    return product(matrix, jnp.concatenate([lines, turned(lines)], axis=0))


def apply_matrix(matrix, other):
    return product(matrix, jnp.concatenate([other, turned_matrix(other)], axis=0))


def tap_pattern(offsets, seg, sweep):
    row = lax.broadcasted_iota(jnp.int32, (8, 128), 0) % TAPS
    out = jnp.zeros((8, 128), jnp.int32)
    for j in range(TAPS):
        out = jnp.where(row == j, offsets[seg, sweep, j], out)
    return out


def selector_of(pattern, coils):
    rows, cols = coils * TAPS, coils * LINES
    lane = lax.broadcasted_iota(jnp.int32, (rows, cols), 1)
    row = lax.broadcasted_iota(jnp.int32, (rows, cols), 0)
    offs = jnp.concatenate([pattern[:, :1]] * (rows // 8), axis=0)
    hit = ((lane & (LINES - 1)) == offs) & ((lane >> 3) == (row >> 2))
    return jnp.where(hit, 1.0, 0.0).astype(BF16)


def choose(index, options):
    out = options[-1]
    for k in reversed(range(len(options) - 1)):
        out = jnp.where(index == k, options[k], out)
    return out


def kernel(
    dims, m_ref, fk_ref, bk_ref, off_ref, fwd_ref, res_ref,
    msend, mrecv, ktall, kcat, amat, lines, offs_own, offs_in,
    gcore, hcore, gx, hx, gy, hy, ucols, urecv,
    offs_s, offs_r, kt_s, kt_r, m_s, m_r, gc_s, gc_r, hc_s, hc_r,
    gx_s, gx_r, hx_s, hx_r, gy_s, gy_r, hy_s, hy_r, u_s, u_r,
):
    ny, nx, nz = dims
    coils = 4 * nz
    rows_own = 4 * LINES
    y, x, q, z = (lax.axis_index(a) for a in (*SEG, "coil"))

    place = (y * nx + x) * 2 + q
    count = ny * nx * 2
    after = lax.rem(place + 1, count)
    before = lax.rem(place + count - 1, count)

    def at_place(p):
        return (lax.div(p, 2 * nx), lax.rem(lax.div(p, 2), nx), lax.rem(p, 2), z)

    def at_z(k):
        return (y, x, q, k)

    def at_x(k):
        return (y, k, q, z)

    def at_y(k):
        return (k, x, q, z)

    partner = (y, x, 1 - q, z)

    def others(mine, size):
        order = sorted(range(1, size), key=lambda i: -min(i, size - i))
        return [lax.rem(mine + i, size) for i in order]

    z_others, x_others, y_others = others(z, nz), others(x, nx), others(y, ny)

    barrier = pltpu.get_barrier_semaphore()
    targets = (
        [at_z(k) for k in z_others] + [at_x(k) for k in x_others] + [at_y(k) for k in y_others]
        + [partner, at_place(after), at_place(before)]
    )
    for t in targets:
        pl.semaphore_signal(barrier, inc=1, device_id=t, device_id_type=MESH)

    offs_own[0] = tap_pattern(off_ref, 0, 0)
    offs_own[1] = tap_pattern(off_ref, 1, 1)
    lane = lax.broadcasted_iota(jnp.int32, (rows_own, 128), 1)
    for seg in range(2):
        for pair in range(nz // 2):
            re = m_ref[seg, 0, :, pair * 128 : pair * 128 + 128]
            im = m_ref[seg, 1, :, pair * 128 : pair * 128 + 128]
            msend[2 * pair, seg] = jnp.where(lane < 64, re, pltpu.roll(im, 64, 1))
            msend[2 * pair + 1, seg] = jnp.where(lane < 64, pltpu.roll(re, 64, 1), im)

    pl.semaphore_wait(barrier, len(targets))

    started = []

    def send(src, dst, ssem, rsem, target):
        copy = pltpu.make_async_remote_copy(
            src_ref=src, dst_ref=dst, send_sem=ssem, recv_sem=rsem,
            device_id=target, device_id_type=MESH,
        )
        copy.start()
        started.append(copy)

    def arrived(dst, ssem, rsem):
        pltpu.make_async_remote_copy(
            src_ref=dst, dst_ref=dst, send_sem=ssem, recv_sem=rsem,
            device_id=partner, device_id_type=MESH,
        ).wait_recv()

    send(offs_own.at[0], offs_in.at[0], offs_s.at[0], offs_r.at[0], at_place(before))
    send(offs_own.at[1], offs_in.at[1], offs_s.at[1], offs_r.at[1], at_place(after))

    def send_kernels(sweep):
        own = bk_ref if sweep else fk_ref
        for k in z_others:
            send(own, ktall.at[sweep, z], kt_s.at[sweep, k], kt_r.at[sweep, z], at_z(k))
        ktall[sweep, z] = own[...]

    send_kernels(0)
    for k in z_others:
        send(msend.at[k], mrecv.at[z], m_s.at[k], m_r.at[z], at_z(k))
    mrecv[z] = msend[z]
    send_kernels(1)

    def build_kernels(sweep):
        for k in z_others:
            arrived(ktall.at[sweep, k], kt_s.at[sweep, k], kt_r.at[sweep, k])
        for seg in range(2):
            parts = []
            for ri in range(2):
                part = jnp.concatenate([ktall[sweep, k, seg, ri] for k in range(nz)], axis=0)
                parts.append(part.T)
            kcat[sweep, seg] = jnp.concatenate(parts, axis=1)

    def exchange(own, ssem, rsem, devices, mine, at):
        for k in devices:
            send(own.at[mine], own.at[mine], ssem.at[k], rsem.at[mine], at(k))

    def gathered(own, ssem, rsem, devices):
        for k in devices:
            arrived(own.at[k], ssem.at[k], rsem.at[k])

    def core_at(k):
        return (y, x, k, z)

    selectors = {}

    def local_maps(sweep):
        first, second = (0, 1) if sweep == 0 else (1, 0)
        inner = selector_of(tap_pattern(off_ref, second, sweep), coils)
        arrived(offs_in.at[sweep], offs_s.at[sweep], offs_r.at[sweep])
        outer = selector_of(offs_in[sweep], coils)
        selectors[sweep] = (inner, outer)
        build_kernels(sweep)
        amat[sweep, 0] = pick(inner, kcat[sweep, first])
        amat[sweep, 1] = pick(outer, kcat[sweep, second])
        gcore[sweep, q] = apply_matrix(amat[sweep, 1], amat[sweep, 0])
        exchange(gcore.at[sweep], gc_s.at[sweep], gc_r.at[sweep], [1 - q], q, core_at)

    def ordered(sweep, size):
        return list(range(size)) if sweep == 0 else list(range(size))[::-1]

    def row_maps(sweep):
        gathered(gcore.at[sweep], gc_s.at[sweep], gc_r.at[sweep], [1 - q])
        early, late = ordered(sweep, 2)
        gx[sweep, x] = apply_matrix(gcore[sweep, late], gcore[sweep, early])
        exchange(gx.at[sweep], gx_s.at[sweep], gx_r.at[sweep], x_others, x, at_x)

    px = {}

    def column_maps(sweep):
        gathered(gx.at[sweep], gx_s.at[sweep], gx_r.at[sweep], x_others)
        order = ordered(sweep, nx)
        through = [gx[sweep, order[0]]]
        for k in order[1:]:
            through.append(apply_matrix(gx[sweep, k], through[-1]))
        gy[sweep, y] = through[-1]
        exchange(gy.at[sweep], gy_s.at[sweep], gy_r.at[sweep], y_others, y, at_y)
        rank = x if sweep == 0 else nx - 1 - x
        px[sweep] = choose(rank, [through[0]] + through[:-1])

    def scan_lines(sweep, first_source, second_source, between):
        rank_q = q if sweep == 0 else 1 - q
        rank_x = x if sweep == 0 else nx - 1 - x
        rank_y = y if sweep == 0 else ny - 1 - y
        early, late = ordered(sweep, 2)
        hcore[sweep, q] = second_source + apply_lines(amat[sweep, 1], first_source)
        exchange(hcore.at[sweep], hc_s.at[sweep], hc_r.at[sweep], [1 - q], q, core_at)
        between[0]()
        gathered(hcore.at[sweep], hc_s.at[sweep], hc_r.at[sweep], [1 - q])
        hx[sweep, x] = hcore[sweep, late] + apply_lines(gcore[sweep, late], hcore[sweep, early])
        exchange(hx.at[sweep], hx_s.at[sweep], hx_r.at[sweep], x_others, x, at_x)
        between[1]()
        gathered(hx.at[sweep], hx_s.at[sweep], hx_r.at[sweep], x_others)
        order = ordered(sweep, nx)
        through = [hx[sweep, order[0]]]
        for k in order[1:]:
            through.append(hx[sweep, k] + apply_lines(gx[sweep, k], through[-1]))
        hy[sweep, y] = through[-1]
        exchange(hy.at[sweep], hy_s.at[sweep], hy_r.at[sweep], y_others, y, at_y)
        in_row = choose(rank_x, [jnp.zeros_like(through[0])] + through[:-1])
        between[2]()
        gathered(gy.at[sweep], gy_s.at[sweep], gy_r.at[sweep], y_others)
        gathered(hy.at[sweep], hy_s.at[sweep], hy_r.at[sweep], y_others)
        order = ordered(sweep, ny)
        rows = [jnp.zeros_like(in_row), hy[sweep, order[0]]]
        for k in order[1:-1]:
            rows.append(hy[sweep, k] + apply_lines(gy[sweep, k], rows[-1]))
        row_in = choose(rank_y, rows)
        chip_in = jnp.where(rank_x == 0, row_in, in_row + apply_lines(px[sweep], row_in))
        core_in = hcore[sweep, early] + apply_lines(gcore[sweep, early], chip_in)
        return jnp.where(rank_q == 0, chip_in, core_in)

    def send_out(sweep):
        for k in z_others:
            at = pl.multiple_of(k * rows_own, rows_own)
            send(
                ucols.at[sweep, :, pl.ds(at, rows_own)], urecv.at[sweep, z],
                u_s.at[sweep, k], u_r.at[sweep, z], at_z(k),
            )
        urecv[sweep, z] = ucols[sweep, :, pl.ds(pl.multiple_of(z * rows_own, rows_own), rows_own)]

    def put_out(sweep, out_ref):
        for k in z_others:
            arrived(urecv.at[sweep, k], u_s.at[sweep, k], u_r.at[sweep, k])
        for seg in range(2):
            for pair in range(nz // 2):
                even, odd = urecv[sweep, 2 * pair, seg], urecv[sweep, 2 * pair + 1, seg]
                cols = slice(pair * 128, pair * 128 + 128)
                out_ref[seg, 0, :, cols] = jnp.where(lane < 64, even, pltpu.roll(odd, 64, 1))
                out_ref[seg, 1, :, cols] = jnp.where(lane < 64, pltpu.roll(even, 64, 1), odd)

    nothing = lambda: None

    local_maps(0)
    row_maps(0)
    for k in z_others:
        arrived(mrecv.at[k], m_s.at[k], m_r.at[k])
    m0 = mrecv[:, 0].reshape(coils * LINES, 128)
    m1 = mrecv[:, 1].reshape(coils * LINES, 128)
    inner, outer = selectors[0]
    b0, b1 = pick(inner, m0), pick(outer, m1)
    lines[0] = b0
    zin = scan_lines(0, b0, b1, [nothing, lambda: column_maps(0), lambda: (local_maps(1), row_maps(1))])
    u0 = apply_lines(kcat[0, 0], zin) + mrecv[:, 0].reshape(coils * LINES, 128)
    z1 = apply_lines(amat[0, 0], zin) + lines[0]
    u1 = apply_lines(kcat[0, 1], z1) + mrecv[:, 1].reshape(coils * LINES, 128)
    ucols[0, 0] = u0
    ucols[0, 1] = u1
    send_out(0)
    inner, outer = selectors[1]
    c1, c0 = pick(inner, u1), pick(outer, u0)
    lines[1] = c1
    win = scan_lines(1, c1, c0, [nothing, lambda: column_maps(1), lambda: put_out(0, fwd_ref)])
    r1 = apply_lines(kcat[1, 1], win) + ucols[0, 1]
    w0 = apply_lines(amat[1, 0], win) + lines[1]
    r0 = apply_lines(kcat[1, 0], w0) + ucols[0, 0]
    ucols[1, 0] = r0
    ucols[1, 1] = r1
    send_out(1)
    put_out(1, res_ref)
    for copy in started:
        copy.wait_send()


def shards(dims, measured, forward_kernel, backward_kernel, line_offsets):
    ny, nx, nz = dims
    coils = 4 * nz
    taps, cols = coils * TAPS, coils * LINES
    flat = measured.reshape(2, 2, 4 * LINES, measured.shape[4])
    by_source = [k.transpose(0, 1, 3, 2) for k in (forward_kernel, backward_kernel)]
    vmem = pl.BlockSpec(memory_space=pltpu.VMEM)
    own = taps // nz
    dma = pltpu.SemaphoreType.DMA
    out = jax.ShapeDtypeStruct(flat.shape, F32)
    forward, result = pl.pallas_call(
        functools.partial(kernel, dims),
        out_shape=(out, out),
        in_specs=[vmem, vmem, vmem, pl.BlockSpec(memory_space=pltpu.SMEM)],
        out_specs=(vmem, vmem),
        scratch_shapes=[
            pltpu.VMEM((nz, 2, 4 * LINES, 128), F32),
            pltpu.VMEM((nz, 2, 4 * LINES, 128), F32),
            pltpu.VMEM((2, nz, 2, 2, own, cols), F32),
            pltpu.VMEM((2, 2, cols, 2 * taps), F32),
            pltpu.VMEM((2, 2, taps, 2 * taps), F32),
            pltpu.VMEM((2, taps, 128), F32),
            pltpu.VMEM((2, 8, 128), jnp.int32),
            pltpu.VMEM((2, 8, 128), jnp.int32),
            pltpu.VMEM((2, 2, taps, 2 * taps), F32),
            pltpu.VMEM((2, 2, taps, 128), F32),
            pltpu.VMEM((2, nx, taps, 2 * taps), F32),
            pltpu.VMEM((2, nx, taps, 128), F32),
            pltpu.VMEM((2, ny, taps, 2 * taps), F32),
            pltpu.VMEM((2, ny, taps, 128), F32),
            pltpu.VMEM((2, 2, cols, 128), F32),
            pltpu.VMEM((2, nz, 2, 4 * LINES, 128), F32),
            dma((2,)), dma((2,)),
            dma((2, nz)), dma((2, nz)),
            dma((nz,)), dma((nz,)),
            dma((2, 2)), dma((2, 2)), dma((2, 2)), dma((2, 2)),
            dma((2, nx)), dma((2, nx)), dma((2, nx)), dma((2, nx)),
            dma((2, ny)), dma((2, ny)), dma((2, ny)), dma((2, ny)),
            dma((2, nz)), dma((2, nz)),
        ],
        compiler_params=pltpu.CompilerParams(collective_id=0, has_side_effects=True),
        name="sweeps",
    )(flat, *by_source, line_offsets)
    return forward.reshape(measured.shape), result.reshape(measured.shape)


def solution(mesh):
    sizes = (4, 4) if mesh.shape["seg"] == 32 else (2, 2)
    dims = (*sizes, mesh.shape["coil"])
    torus = Mesh(mesh.devices.reshape(*sizes, 2, dims[2]), (*SEG, "coil"))
    return jax.shard_map(
        functools.partial(shards, dims),
        mesh=torus,
        in_specs=(
            P(SEG, None, "coil", None, None),
            P(SEG, None, None, "coil"),
            P(SEG, None, None, "coil"),
            P(SEG, None, None),
        ),
        out_specs=(P(SEG, None, "coil", None, None), P(SEG, None, "coil", None, None)),
        check_vma=False,
    )
```
